32 devices in a mesh: cell: 8 (over z, x), seq: 4 (over y, core).
Axes of the slice: x: 2, y: 2, z: 4, core: 2. Of those that a mesh axis runs over, the one named last changes fastest.
Arguments:
- cells_in: bfloat16 [8, 1024, 1120], P('cell', 'seq'), may hold values from -6 to 6
- dataset_ids: int32 [8], P('cell'), may hold values from 0 to 15
- cell_lengths: int32 [8], P('cell'), may hold values from 512 to 1024, as said below
- table: float32 [16, 1120], replicated, may hold values from -3 to 3
- wqkv: bfloat16 [1120, 3360], P('seq'), may hold values from -0.25 to 0.25
- bq: float32 [1120], replicated, may hold values from -3 to 3
- bv: float32 [1120], replicated, may hold values from -3 to 3
- wout: bfloat16 [1120, 1120], P('seq'), may hold values from -0.5 to 0.5
- bout: float32 [1120], replicated, may hold values from -2 to 2
- gain1: float32 [1120], replicated, may hold values from 0.1 to 1.9
- shift1: float32 [1120], replicated, may hold values from -2 to 2
- gain2: float32 [1120], replicated, may hold values from 0.1 to 1.9
- shift2: float32 [1120], replicated, may hold values from -2 to 2
- wup: bfloat16 [1120, 4480], P(None, 'cell'), may hold values from -0.1875 to 0.1875
- bup: float32 [4480], replicated, may hold values from -2 to 2
- wdown: bfloat16 [4480, 1120], P('cell'), may hold values from -0.09375 to 0.09375
- bdown: float32 [1120], replicated, may hold values from -2 to 2
- out_grad: bfloat16 [8, 1024, 1120], P('cell', 'seq'), may hold values from -6 to 6
Outputs:
- cells_out: bfloat16 [8, 1024, 1120], P('cell', 'seq')
- cells_grad: bfloat16 [8, 1024, 1120], P('cell', 'seq')
- grad_table: float32 [16, 1120], P(None, 'seq')
- grad_wqkv: float32 [1120, 3360], P('seq')
- grad_bq: float32 [1120], P('seq')
- grad_bv: float32 [1120], P('seq')
- grad_wout: float32 [1120, 1120], P('seq')
- grad_bout: float32 [1120], P('seq')
- grad_gain1: float32 [1120], P('seq')
- grad_shift1: float32 [1120], P('seq')
- grad_gain2: float32 [1120], P('seq')
- grad_shift2: float32 [1120], P('seq')
- grad_wup: float32 [1120, 4480], P(None, 'cell')
- grad_bup: float32 [4480], P('seq')
- grad_wdown: float32 [4480, 1120], P('cell')
- grad_bdown: float32 [1120], P('seq')
The draws below stay inside these ranges and needn't reach their ends.
Inputs may be any that keep to these rules, and one draw needn't show every extreme that they name: `cell_lengths`: some cell has exactly 1024 live positions.
All inputs are finite; a program needn't handle non-finite values.
Results may differ from the reference program's by a relative error of at most 0.015.
Values may be sent and summed in bfloat16 or wider, within the bound.
A program may use at most 256 MiB of HBM per device.

```python
import math
import jax
import jax.numpy as jnp
import numpy as np
from jax import lax

D = 1120
HEADS = 20
HEAD_DIM = 56
FF = 4480
DATASETS = 16
SLOTS = 1024
CELLS = 8


def draw_cell_lengths(key, part):
    folded = jax.random.fold_in(key, 11)
    first_key, second_key = jax.random.split(folded)
    drawn = jax.random.randint(first_key, (CELLS,), SLOTS // 2, SLOTS + 1)
    longest = jax.random.randint(second_key, (), 0, CELLS)
    return jnp.where(jnp.arange(CELLS) == longest, SLOTS, drawn).astype(jnp.int32)


def with_ends(values, own_key, least, top_value):
    spot = [jax.random.randint(jax.random.fold_in(own_key, axis), (), 0, length) for axis, length in enumerate(values.shape)]
    widest = values.shape.index(max(values.shape))
    beside = spot[:widest] + [(spot[widest] + 1) % values.shape[widest]] + spot[widest + 1:]
    return values.at[tuple(spot)].set(least).at[tuple(beside)].set(top_value)


def level_of(own_key, dims, shards, least, largest):
    def one(position, shards_of):
        steps = jax.random.uniform(jax.random.fold_in(jax.random.fold_in(own_key, 6), position), (shards_of,), jnp.float32, least / len(shards), largest / len(shards))
        return jnp.repeat(jnp.exp(steps), dims[position] // shards_of).reshape((-1,) + (1,) * (len(dims) - position - 1))

    level = one(*shards[0])
    for cut in shards[1:]:
        level = level * one(*cut)
    return level


def rank_table(number_of, lean):
    portions = [(1 << 20) // math.isqrt(grade ** lean) + 1 for grade in range(1, number_of + 1)]
    scale = 1 + sum(portions) // (1 << 30)
    return np.cumsum(np.array([max(1, weight // scale) for weight in portions]))


def ranked_ids(rng, shape, amount, lean):
    listing = rank_table(amount, lean)
    pick = jax.random.randint(jax.random.fold_in(rng, 1), shape, 0, int(listing[amount - 1]))
    grade = jnp.searchsorted(jnp.asarray(listing, jnp.int32), pick, side="right")
    return jax.random.permutation(jax.random.fold_in(rng, 2), amount)[grade].astype(jnp.int32)


def bell_draw(key, dims, scale, reach, cuts=(), kind=jnp.bfloat16):
    values = jax.random.normal(key, dims, jnp.float32) * scale
    if len(cuts) > 0:
        values = level_of(key, dims, cuts, -0.22, 0.18) * values
    return jnp.clip(values, min=-reach, max=reach).astype(kind)


def setup_inputs(seed: int = 0) -> dict:
    key_of = jax.random.split(jax.random.key(seed), 19)
    return {
        "cells_in": bell_draw(key_of[0], (CELLS, SLOTS, D), 1.0, 6.0, ((0, 8), (1, 4))),
        "dataset_ids": with_ends(ranked_ids(key_of[1], (CELLS,), DATASETS, 2), jax.random.fold_in(key_of[1], 3), 0, DATASETS - 1).astype(jnp.int32),
        "cell_lengths": draw_cell_lengths(jax.random.fold_in(key_of[18], 71), 0),
        "table": bell_draw(key_of[3], (DATASETS, D), 0.5, 3.0, (), jnp.float32),
        "wqkv": bell_draw(key_of[4], (D, 3 * D), (D // 2) ** -0.5, 0.25, ((0, 4),)),
        "bq": bell_draw(key_of[5], (D,), 0.5, 3.0, (), jnp.float32),
        "bv": bell_draw(key_of[6], (D,), 0.5, 3.0, (), jnp.float32),
        "wout": bell_draw(key_of[7], (D, D), (D // 8) ** -0.5, 0.5, ((0, 4),)),
        "bout": bell_draw(key_of[8], (D,), 0.3, 2.0, (), jnp.float32),
        "gain1": jnp.clip(1.0 + 0.18 * jax.random.normal(key_of[9], (D,), jnp.float32), 0.1, 1.9),
        "shift1": bell_draw(key_of[10], (D,), 0.3, 2.0, (), jnp.float32),
        "gain2": jnp.clip(1.0 + 0.18 * jax.random.normal(key_of[11], (D,), jnp.float32), 0.1, 1.9),
        "shift2": bell_draw(key_of[12], (D,), 0.3, 2.0, (), jnp.float32),
        "wup": bell_draw(key_of[13], (D, FF), D ** -0.5, 0.1875, ((1, 8),)),
        "bup": bell_draw(key_of[14], (FF,), 0.3, 2.0, (), jnp.float32),
        "wdown": bell_draw(key_of[15], (FF, D), FF ** -0.5, 0.09375, ((0, 8),)),
        "bdown": bell_draw(key_of[16], (D,), 0.3, 2.0, (), jnp.float32),
        "out_grad": bell_draw(key_of[17], (CELLS, SLOTS, D), 1.0, 6.0, ((0, 8), (1, 4))),
    }


@jax.custom_vjp
def low(v):
    return lax.optimization_barrier(v.astype(jnp.bfloat16)).astype(jnp.float32)

@jax.custom_vjp
def low_back(v):
    return v

def low_keep(v):
    return (low(v), None)

def low_pass(kept, grad):
    return (grad,)

def back_keep(v):
    return (v, None)

def back_low(kept, grad):
    return (low(grad),)
low.defvjp(low_keep, low_pass)
low_back.defvjp(back_keep, back_low)

def matmul_high(left, right):
    return jnp.dot(left, right, precision=lax.Precision.HIGHEST, preferred_element_type=jnp.float32)

def norm_rows(hidden, gain, shift):
    centre = hidden - lax.optimization_barrier(jnp.mean(hidden, axis=-1, keepdims=True))
    spread = lax.optimization_barrier(jnp.mean(centre * centre, axis=-1, keepdims=True))
    return centre * lax.rsqrt(spread + 1e-05) * gain + shift

def attend_cell(query_all, key_all, value_all, length):
    slot_count = query_all.shape[0]
    row_block = min(512, slot_count)
    score_scale = 1.0 / math.sqrt(HEAD_DIM)
    key_pos = jnp.arange(slot_count, dtype=jnp.int32)

    def one_block(operands):
        queries, first_row = operands
        query_pos = first_row + jnp.arange(row_block, dtype=jnp.int32)
        scores = jnp.einsum('qhd,khd->hqk', queries, key_all, precision=lax.Precision.HIGHEST)
        scores = low_back(scores * score_scale)
        visible = (key_pos[None, :] <= query_pos[:, None]) & (key_pos[None, :] < length)
        scores = jnp.where(visible[None], scores, -1e+30)
        prob_low = low(jax.nn.softmax(scores, axis=-1))
        return jnp.einsum('hqk,khd->qhd', prob_low, value_all, precision=lax.Precision.HIGHEST)
    starts = jnp.arange(slot_count // row_block, dtype=jnp.int32) * row_block
    blocks = lax.map(jax.checkpoint(one_block), (query_all.reshape(slot_count // row_block, row_block, HEADS, HEAD_DIM), starts))
    return blocks.reshape(slot_count, HEADS * HEAD_DIM)

def block_layer(params, cell_in, table_row, length):
    wqkv, bq, bv, wout, bout, gain1, shift1, gain2, shift2, wup, bup, wdown, bdown = params
    resid_in = cell_in + table_row
    normed1 = low(norm_rows(resid_in, gain1, shift1))
    qkv = matmul_high(normed1, wqkv)
    query_all = low_back(low(qkv[:, :D] + bq))
    key_all = low_back(low(qkv[:, D:2 * D]))
    value_all = low_back(low(qkv[:, 2 * D:] + bv))
    slot_count = cell_in.shape[0]
    context = attend_cell(query_all.reshape(slot_count, HEADS, HEAD_DIM), key_all.reshape(slot_count, HEADS, HEAD_DIM), value_all.reshape(slot_count, HEADS, HEAD_DIM), length)
    context = low_back(low(context))
    attn_branch = low_back(matmul_high(context, wout) + bout)
    resid_mid = resid_in + attn_branch
    normed2 = low(norm_rows(resid_mid, gain2, shift2))
    up_rows = low_back(matmul_high(normed2, wup) + bup)
    act_rows = low(jax.nn.gelu(up_rows, approximate=True))
    ffn_branch = low_back(matmul_high(act_rows, wdown) + bdown)
    return resid_mid + ffn_branch

def reference(cells_in, dataset_ids, cell_lengths, table, wqkv, bq, bv, wout, bout, gain1, shift1, gain2, shift2, wup, bup, wdown, bdown, out_grad):
    params = tuple((p.astype(jnp.float32) for p in (wqkv, bq, bv, wout, bout, gain1, shift1, gain2, shift2, wup, bup, wdown, bdown)))
    table_wide = table.astype(jnp.float32)
    zero_grads = tuple((jnp.zeros_like(p) for p in params))

    def cell_step(carry, item):
        grad_sums, table_sum = carry
        cell_in, cell_cot, ident, length = item
        picked = (jnp.arange(DATASETS, dtype=jnp.int32) == ident).astype(jnp.float32)

        def whole(param_set, cell_wide, table_all):
            table_row = matmul_high(picked[None, :], table_all)
            return block_layer(param_set, cell_wide, table_row, length)
        result, pullback = jax.vjp(whole, params, cell_in.astype(jnp.float32), table_wide)
        grad_params, grad_cell, grad_tab = pullback(cell_cot.astype(jnp.float32))
        grad_sums = jax.tree.map(lambda first, second: first + second, grad_sums, grad_params)
        return ((grad_sums, table_sum + grad_tab), (result.astype(jnp.bfloat16), grad_cell.astype(jnp.bfloat16)))
    (grads, grad_table), (outputs, input_grads) = lax.scan(cell_step, (zero_grads, jnp.zeros_like(table_wide)), (cells_in, out_grad, dataset_ids, cell_lengths))
    return (outputs, input_grads, grad_table, grads[0], grads[1], grads[2], grads[3], grads[4], grads[5], grads[6], grads[7], grads[8], grads[9], grads[10], grads[11], grads[12])
```

```python
import math

import jax
import jax.numpy as jnp
from jax import lax
from jax.sharding import Mesh
from jax.sharding import PartitionSpec as P

HEAD_DIM = 56


norm_eps = 1e-05


CELL = ("outer", "pair")
SEQ = ("far", "core")
WEIGHT = ("outer", "far", "core")


def swapped(x):
    return lax.ppermute(x, "pair", [(0, 1), (1, 0)])


def product(left, right):
    return jnp.dot(left, right, preferred_element_type=jnp.float32)


def left_inner(left, right):
    return lax.dot_general(
        left, right, (((0,), (0,)), ((), ())), preferred_element_type=jnp.float32
    )


def right_inner(left, right):
    return lax.dot_general(
        left, right, (((1,), (1,)), ((), ())), preferred_element_type=jnp.float32
    )


def norm_forward(hidden, gain, shift):
    centre = hidden - jnp.mean(hidden, axis=-1, keepdims=True)
    inverse = lax.rsqrt(jnp.mean(centre * centre, axis=-1, keepdims=True) + norm_eps)
    unit_rows = centre * inverse
    return (unit_rows * gain + shift, unit_rows, inverse)


def norm_backward(grad_rows, unit_rows, inverse, gain):
    scaled = grad_rows * gain
    inside = (
        scaled
        - jnp.mean(scaled, axis=-1, keepdims=True)
        - unit_rows * jnp.mean(scaled * unit_rows, axis=-1, keepdims=True)
    )
    return (inside * inverse, jnp.sum(grad_rows * unit_rows, axis=0), jnp.sum(grad_rows, axis=0))


def block_scores(queries, keys_used, first_row, length, score_scale):
    row_count = queries.shape[0]
    key_count = keys_used.shape[0]
    scores = (
        jnp.einsum("qhd,khd->hqk", queries, keys_used, preferred_element_type=jnp.float32)
        * score_scale
    )
    query_pos = first_row + lax.broadcasted_iota(jnp.int32, (row_count, key_count), 0)
    key_pos = lax.broadcasted_iota(jnp.int32, (row_count, key_count), 1)
    visible = (key_pos <= query_pos) & (key_pos < length)
    return jnp.where(visible[None], scores, -1e30)


def attend_forward(query_heads, key_heads, value_heads, length, row_block, score_scale):
    slot_count = query_heads.shape[0]
    outputs = []
    logsums = []
    for block_idx in range(slot_count // row_block):
        first_row = block_idx * row_block
        key_count = first_row + row_block
        scores = block_scores(
            query_heads[first_row:key_count], key_heads[:key_count], first_row, length, score_scale
        )
        highest = jnp.max(scores, axis=-1, keepdims=True)
        weights = jnp.exp(scores - highest)
        denominator = jnp.sum(weights, axis=-1, keepdims=True)
        prob_low = (weights / denominator).astype(jnp.bfloat16)
        outputs.append(
            jnp.einsum(
                "hqk,khd->qhd",
                prob_low,
                value_heads[:key_count],
                preferred_element_type=jnp.float32,
            )
        )
        logsums.append(highest + jnp.log(denominator))
    return (jnp.concatenate(outputs, axis=0), logsums)


def attend_backward(
    query_heads, key_heads, value_heads, grad_heads, logsums, length, row_block, score_scale
):
    slot_count = query_heads.shape[0]
    grad_query = []
    grad_key = jnp.zeros(key_heads.shape, jnp.float32)
    grad_value = jnp.zeros(value_heads.shape, jnp.float32)
    for block_idx in range(slot_count // row_block):
        first_row = block_idx * row_block
        key_count = first_row + row_block
        queries = query_heads[first_row:key_count]
        grads_here = grad_heads[first_row:key_count]
        scores = block_scores(queries, key_heads[:key_count], first_row, length, score_scale)
        prob_full = jnp.exp(scores - logsums[block_idx])
        prob_low = prob_full.astype(jnp.bfloat16)
        grad_prob = jnp.einsum(
            "qhd,khd->hqk", grads_here, value_heads[:key_count], preferred_element_type=jnp.float32
        )
        grad_value = grad_value.at[:key_count].add(
            jnp.einsum("hqk,qhd->khd", prob_low, grads_here, preferred_element_type=jnp.float32)
        )
        row_inner = jnp.sum(prob_full * grad_prob, axis=-1, keepdims=True)
        grad_score = (prob_full * (grad_prob - row_inner)).astype(jnp.bfloat16)
        grad_query.append(
            jnp.einsum(
                "hqk,khd->qhd",
                grad_score,
                key_heads[:key_count],
                preferred_element_type=jnp.float32,
            )
            * score_scale
        )
        grad_key = grad_key.at[:key_count].add(
            jnp.einsum("hqk,qhd->khd", grad_score, queries, preferred_element_type=jnp.float32)
            * score_scale
        )
    return (jnp.concatenate(grad_query, axis=0), grad_key, grad_value)


def shards(
    cells_in,
    dataset_ids,
    cell_lengths,
    table,
    wqkv,
    bq,
    bv,
    wout,
    bout,
    gain1,
    shift1,
    gain2,
    shift2,
    wup,
    bup,
    wdown,
    bdown,
    out_grad,
):
    low = jnp.bfloat16
    seq_count = lax.axis_size(SEQ)
    outer_count = lax.axis_size("outer")
    group = lax.axis_index(SEQ)
    pair = lax.axis_index("pair")
    local_rows = cells_in.shape[1]
    width = cells_in.shape[2]
    slot_count = local_rows * seq_count
    group_width = width // seq_count
    hidden = wup.shape[1]
    heads_here = group_width // HEAD_DIM
    row_block = min(512, slot_count)
    score_scale = 1.0 / math.sqrt(HEAD_DIM)
    length = cell_lengths[0]

    dataset_pick = (
        lax.broadcasted_iota(jnp.int32, (1, table.shape[0]), 1) == dataset_ids[0]
    ).astype(jnp.float32)
    table_row = jnp.dot(
        dataset_pick, table, precision=lax.Precision.HIGHEST, preferred_element_type=jnp.float32
    )
    resid_in = cells_in[0].astype(jnp.float32) + table_row
    normed1, unit1, inverse1 = norm_forward(resid_in, gain1, shift1)
    normed1_all = lax.all_gather(normed1.astype(low), SEQ, axis=0, tiled=True)
    group_weights = lax.all_to_all(
        wqkv.reshape(wqkv.shape[0], 3, seq_count, group_width),
        SEQ,
        split_axis=2,
        concat_axis=0,
        tiled=True,
    ).reshape(width, 3 * group_width)
    wout_full = lax.all_gather(wout, SEQ, axis=0, tiled=True)

    own_part = jnp.concatenate([wup.T, wdown], axis=0)
    part_rows = own_part.shape[0] // seq_count
    own_part = lax.dynamic_slice_in_dim(own_part, group * part_rows, part_rows, axis=0)
    ff_weights = lax.all_gather(own_part, WEIGHT, axis=0, tiled=True)
    ff_weights = ff_weights.reshape(outer_count, 2, hidden, width)
    wup_rows = ff_weights[:, 0].reshape(outer_count * hidden, width)
    wdown_rows = ff_weights[:, 1].reshape(outer_count * hidden, width)
    bup_here = lax.dynamic_index_in_dim(
        bup.reshape(outer_count, 2, hidden), pair, axis=1, keepdims=False
    ).reshape(-1)

    grad_out = out_grad[0]
    grad_out_both = jnp.concatenate([grad_out, swapped(grad_out)], axis=0)

    bias_here = lax.dynamic_slice_in_dim(
        jnp.stack([bq, jnp.zeros_like(bq), bv]), group * group_width, group_width, axis=1
    )
    qkv_heads = (product(normed1_all, group_weights) + bias_here.reshape(-1)).astype(low)
    query_heads, key_heads, value_heads = (
        qkv_heads[:, third * group_width : (third + 1) * group_width].reshape(
            slot_count, heads_here, HEAD_DIM
        )
        for third in range(3)
    )
    context, logsums = attend_forward(
        query_heads, key_heads, value_heads, length, row_block, score_scale
    )
    context_low = context.astype(low).reshape(slot_count, 1, group_width)
    context_rows = lax.all_to_all(
        context_low, SEQ, split_axis=0, concat_axis=1, tiled=True
    ).reshape(local_rows, width)
    resid_mid = resid_in + product(context_rows, wout_full) + bout
    normed2, unit2, inverse2 = norm_forward(resid_mid, gain2, shift2)
    normed2_low = normed2.astype(low)

    normed2_both = jnp.concatenate([normed2_low, swapped(normed2_low)], axis=0)
    up_rows = right_inner(normed2_both, wup_rows) + bup_here
    act_low = jax.nn.gelu(up_rows, approximate=True).astype(low)
    down_both = product(act_low, wdown_rows)
    down_here = down_both[:local_rows] + swapped(down_both[local_rows:].astype(low)).astype(
        jnp.float32
    )
    cells_out = (resid_mid + down_here + bdown).astype(low)[None]
    grad_rows = grad_out.astype(jnp.float32)
    grad_bdown = jnp.sum(grad_rows, axis=0)
    grad_wdown = left_inner(act_low, grad_out_both)
    grad_act = right_inner(grad_out_both, wdown_rows)
    gelu_pull = jax.vjp(lambda values: jax.nn.gelu(values, approximate=True), up_rows)[1]
    grad_up_low = gelu_pull(grad_act)[0].astype(low)
    grad_bup = jnp.sum(grad_up_low.astype(jnp.float32), axis=0)
    grad_wup = left_inner(grad_up_low, normed2_both)
    grad_norm2_both = product(grad_up_low, wup_rows)
    grad_norm2 = grad_norm2_both[:local_rows] + swapped(
        grad_norm2_both[local_rows:].astype(low)
    ).astype(jnp.float32)
    ff_grads = jnp.stack(
        [
            grad_wup.astype(low).reshape(outer_count, hidden, width),
            grad_wdown.astype(low).reshape(outer_count, hidden, width),
        ],
        axis=1,
    ).reshape(outer_count * 2 * hidden, width)
    ff_part = lax.psum_scatter(ff_grads, WEIGHT, scatter_dimension=0, tiled=True)
    ff_total = lax.all_gather(ff_part, SEQ, axis=0, tiled=True).astype(jnp.float32)
    total_up = ff_total[:hidden].T
    total_down = ff_total[hidden:]

    back_second, grad_gain2, grad_shift2 = norm_backward(grad_norm2, unit2, inverse2, gain2)
    grad_mid = grad_rows + back_second
    grad_mid_low = grad_mid.astype(low)
    grad_bout = jnp.sum(grad_mid_low.astype(jnp.float32), axis=0)
    grad_context = right_inner(grad_mid_low, wout_full).astype(low)
    grad_context_heads = lax.all_to_all(
        grad_context.reshape(local_rows, seq_count, group_width),
        SEQ,
        split_axis=1,
        concat_axis=0,
        tiled=True,
    ).reshape(slot_count, heads_here, HEAD_DIM)
    grad_wout = left_inner(context_rows, grad_mid_low)
    total_wout = lax.psum(
        lax.psum_scatter(grad_wout.astype(low), SEQ, scatter_dimension=0, tiled=True), CELL
    ).astype(jnp.float32)
    grad_query, grad_key, grad_value = attend_backward(
        query_heads,
        key_heads,
        value_heads,
        grad_context_heads,
        logsums,
        length,
        row_block,
        score_scale,
    )
    grad_qkv = jnp.concatenate(
        [part.reshape(slot_count, group_width) for part in (grad_query, grad_key, grad_value)],
        axis=1,
    ).astype(low)
    grad_norm1 = lax.psum_scatter(
        right_inner(grad_qkv, group_weights).astype(low), SEQ, scatter_dimension=0, tiled=True
    ).astype(jnp.float32)
    grad_wqkv = left_inner(normed1_all, grad_qkv).astype(low)
    grad_wqkv = lax.all_to_all(
        grad_wqkv.reshape(seq_count, group_width, 3 * group_width),
        SEQ,
        split_axis=0,
        concat_axis=0,
        tiled=True,
    )
    total_wqkv = lax.psum(grad_wqkv, CELL).astype(jnp.float32)
    total_wqkv = jnp.transpose(
        total_wqkv.reshape(seq_count, group_width, 3, group_width), (1, 2, 0, 3)
    ).reshape(group_width, 3 * width)
    grad_qkv_sums = jnp.sum(grad_qkv.astype(jnp.float32), axis=0)
    back_first, grad_gain1, grad_shift1 = norm_backward(grad_norm1, unit1, inverse1, gain1)
    grad_in = grad_mid + back_first
    cells_grad = grad_in.astype(low)[None]

    row_sums = jnp.stack(
        [
            jnp.sum(grad_in, axis=0),
            grad_bout,
            grad_gain1,
            grad_shift1,
            grad_gain2,
            grad_shift2,
            grad_bdown,
        ]
    )
    slot = (jnp.arange(2)[:, None] == pair).astype(jnp.float32)
    bup_slots = (slot * grad_bup.reshape(outer_count, 1, hidden)).reshape(seq_count, 1, -1)
    table_rows = jnp.transpose(dataset_pick) * row_sums[:1]
    own_group = (jnp.arange(seq_count)[:, None] == group).astype(jnp.float32)
    q_sums, v_sums = grad_qkv_sums[:group_width], grad_qkv_sums[2 * group_width :]
    small = jnp.concatenate(
        [
            jnp.concatenate([table_rows, row_sums[1:]])
            .reshape(-1, seq_count, group_width)
            .transpose(1, 0, 2)
            .reshape(seq_count, -1),
            own_group * q_sums,
            own_group * v_sums,
            bup_slots.reshape(seq_count, -1),
        ],
        axis=1,
    )
    small = lax.psum(small, ("outer", "pair", "far", "core"))
    small = lax.dynamic_index_in_dim(small, group, axis=0, keepdims=False)
    count = table.shape[0] + 6
    rows = small[: count * group_width].reshape(count, group_width)
    total_table = rows[: table.shape[0]]
    total_bout, total_gain1, total_shift1, total_gain2, total_shift2, total_bdown = rows[
        table.shape[0] :
    ]
    rest = small[count * group_width :]
    total_bq, total_bv, total_bup = (
        rest[:group_width],
        rest[group_width : 2 * group_width],
        rest[2 * group_width :],
    )
    return (
        cells_out,
        cells_grad,
        total_table,
        total_wqkv,
        total_bq,
        total_bv,
        total_wout,
        total_bout,
        total_gain1,
        total_shift1,
        total_gain2,
        total_shift2,
        total_up,
        total_bup,
        total_down,
        total_bdown,
    )


def solution(mesh):
    cells, seqs = mesh.devices.shape
    fine = Mesh(
        mesh.devices.reshape(cells // 2, 2, seqs // 2, 2), ("outer", "pair", "far", "core")
    )
    return jax.shard_map(
        shards,
        mesh=fine,
        in_specs=(
            P(CELL, SEQ, None),
            P(CELL),
            P(CELL),
            P(),
            P(SEQ, None),
            P(),
            P(),
            P(SEQ, None),
            P(),
            P(),
            P(),
            P(),
            P(),
            P(None, CELL),
            P(),
            P(CELL, None),
            P(),
            P(CELL, SEQ, None),
        ),
        out_specs=(
            P(CELL, SEQ, None),
            P(CELL, SEQ, None),
            P(None, SEQ),
            P(SEQ, None),
            P(SEQ),
            P(SEQ),
            P(SEQ, None),
            P(SEQ),
            P(SEQ),
            P(SEQ),
            P(SEQ),
            P(SEQ),
            P(None, CELL),
            P(SEQ),
            P(CELL, None),
            P(SEQ),
        ),
        check_vma=False,
    )
```
